32 devices in a mesh: row: 8 (over z, x), col: 4 (over y, core).
Axes of the slice: x: 2, y: 2, z: 4, core: 2. Of those that a mesh axis runs over, the one named last changes fastest.
Arguments:
- hub_seeds: bfloat16 [192, 64, 128], P('row'), may hold values from -6 to 6
- tile_blocks: bfloat16 [8192, 128, 128], P(('row', 'col')), may hold values from -8 to 8
- tile_rows: int32 [8192], P(('row', 'col')), may hold values from 0 to 127, as said below
- tile_cols: int32 [8192], P(('row', 'col')), may hold values from 0 to 127, as said below
- tile_count: int32 [32], P(('row', 'col')), may hold values from 64 to 256, as said below
- row_blocks: int32 [8], replicated, may hold values from 8 to 24, as said below
Outputs:
- authority: bfloat16 [128, 64, 128], P(('row', 'col'))
- hub_scores: bfloat16 [192, 64, 128], P('row')
The draws below stay inside these ranges and needn't reach their ends.
Inputs may be any that keep to these rules, and one draw needn't show every extreme that they name: Row range r covers row blocks starts[r] to starts[r] + row_blocks[r] - 1, the ranges in order and together all 128 blocks; the longest range has exactly 24 blocks in every draw. `tile_rows`: every tile of a device lies in the row range of the device's row index; no pair of row block and column block repeats within a device. `tile_cols`: A device with column index c holds only column blocks b with (b // 4) % 4 == c. The live tiles of a device are its first tile_count slots; some device has all 256 slots live in every draw.
All inputs are finite; a program needn't handle non-finite values.
Results may differ from the reference program's by a relative error of at most 0.02.
Values may be sent and summed in bfloat16 or wider, within the bound.
A program may use at most 192 MiB of HBM per device.

```python
import jax
import jax.numpy as jnp
from jax import lax

K = 64
TB = 128
ITERS = 2
RB_DEV = 16
ROWDEV = 8
COLDEV = 4
NB = 128
HOSTS = 16384
LMAX = 24
COLUMN_BLOCKS_SET = 32
GROUP = 4
TILE_DEV = 256


def tile_layout(key):
    base_key = jax.random.fold_in(key, 4127)
    key_len, key_pick, key_sign, key_perm, key_count, key_full, key_popular = jax.random.split(base_key, 7)
    half_len = RB_DEV // 2
    pair_count = ROWDEV // 2
    shifts = jax.random.randint(key_len, (pair_count,), -half_len, half_len + 1)
    forced = jax.random.randint(key_pick, (), 0, pair_count)
    flip_sign = jax.random.randint(key_sign, (), 0, 2) * 2 - 1
    shifts = jnp.where(jnp.arange(pair_count) == forced, half_len * flip_sign, shifts)
    lengths = jnp.stack([RB_DEV - shifts, RB_DEV + shifts], axis=1).reshape(ROWDEV).astype(jnp.int32)
    starts = jnp.cumsum(lengths) - lengths
    device_count = ROWDEV * COLDEV
    lattice_size = LMAX * COLUMN_BLOCKS_SET
    device_rows = jnp.arange(device_count) // COLDEV
    device_cols = jnp.arange(device_count) % COLDEV
    device_keys = jax.random.split(key_perm, device_count)
    popular_run = jax.random.randint(key_popular, (), 0, ROWDEV)
    prefers = jnp.arange(device_count) % 2 == 0

    def choose(dev_key, span_length, prefer):
        pairing_index = jax.random.permutation(dev_key, lattice_size)
        location_list = jnp.arange(lattice_size)
        favored_hosts = (pairing_index % COLUMN_BLOCKS_SET // GROUP == popular_run) & prefer
        extra_credit = jnp.where(favored_hosts, lattice_size, 0)
        rating_values = jnp.where(pairing_index // COLUMN_BLOCKS_SET < span_length, lattice_size - location_list + extra_credit, -1 - location_list)
        best_vals, best_idx = lax.top_k(rating_values, TILE_DEV)
        return pairing_index[best_idx]
    chosen = jax.vmap(choose)(device_keys, lengths[device_rows], prefers)
    row_list = starts[device_rows][:, None] + chosen // COLUMN_BLOCKS_SET
    col_local = chosen % COLUMN_BLOCKS_SET
    col_list = (col_local // GROUP * COLDEV + device_cols[:, None]) * GROUP + col_local % GROUP
    counts = TILE_DEV // jax.random.randint(key_count, (device_count,), 1, 5)
    full_dev = jax.random.randint(key_full, (), 0, device_count)
    counts = jnp.where(jnp.arange(device_count) == full_dev, TILE_DEV, counts)
    return (lengths, row_list.reshape(-1).astype(jnp.int32), col_list.reshape(-1).astype(jnp.int32), counts.astype(jnp.int32))


def draw_tile_blocks(key, part):
    fan_value = max(1, TB * TILE_DEV * COLDEV // (512 * RB_DEV))
    base_scale = float(fan_value) ** (-0.5)
    tile_total = ROWDEV * COLDEV * TILE_DEV
    owner_row = (jnp.arange(tile_total) // (COLDEV * TILE_DEV)).astype(jnp.float32)
    position = owner_row / float(ROWDEV - 1)
    draw_key = jax.random.fold_in(key, 9311)
    scales = base_scale * (0.5 + 1.5 * position)
    values = jnp.clip(jax.random.normal(draw_key, (tile_total, TB, TB), jnp.float32), -6.0, 6.0)
    return jnp.clip(values * scales[:, None, None], -8.0, 8.0).astype(jnp.bfloat16)


def draw_row_blocks(key, part):
    return tile_layout(key)[0]


def draw_tile_rows(key, part):
    return tile_layout(key)[1]


def draw_tile_cols(key, part):
    return tile_layout(key)[2]


def draw_tile_count(key, part):
    return tile_layout(key)[3]


def steps_of(own_key, dims, pieces, smallest, top_value):
    factor_of = 1.0
    for dim, parts in pieces:
        steps = jax.random.uniform(jax.random.fold_in(jax.random.fold_in(own_key, 6), dim), (parts,), jnp.float32, smallest / len(pieces), top_value / len(pieces))
        factor_of = factor_of * jnp.repeat(jnp.exp(steps), dims[dim] // parts).reshape((-1,) + (1,) * (len(dims) - 1 - dim))
    return factor_of


def gaussian(stream_key, shape, width, reach, cuts=(), held_as=jnp.bfloat16):
    entries = jax.random.normal(stream_key, shape, jnp.float32) * width
    if len(cuts) > 0:
        entries = steps_of(stream_key, shape, cuts, -0.22, 0.18) * entries
    return jnp.clip(entries, min=-reach, max=reach).astype(held_as)


def setup_inputs(seed: int = 0) -> dict:
    seeds = jax.random.split(jax.random.key(seed), 7)
    hub_seeds = gaussian(seeds[0], (ROWDEV * LMAX, K, TB), 1.0, 6.0, ((0, 8),))
    tile_blocks = draw_tile_blocks(jax.random.fold_in(seeds[6], 71), 0)
    tile_rows = draw_tile_rows(jax.random.fold_in(seeds[6], 71), 0)
    tile_cols = draw_tile_cols(jax.random.fold_in(seeds[6], 71), 0)
    tile_count = draw_tile_count(jax.random.fold_in(seeds[6], 71), 0)
    row_blocks = draw_row_blocks(jax.random.fold_in(seeds[6], 71), 0)
    return {"hub_seeds": hub_seeds, "tile_blocks": tile_blocks, "tile_rows": tile_rows, "tile_cols": tile_cols, "tile_count": tile_count, "row_blocks": row_blocks}


def normalize(raw_scores):
    squares = lax.optimization_barrier(jnp.sum(raw_scores * raw_scores, axis=(0, 2)))
    factor = 1.0 / jnp.sqrt(squares / HOSTS + 1.0)
    return (raw_scores * factor[None, :, None]).astype(jnp.bfloat16)

def rounded_partial(partial_value):
    return lax.optimization_barrier(partial_value.astype(jnp.bfloat16)).astype(jnp.float32)

def reference(hub_seeds, tile_blocks, tile_rows, tile_cols, tile_count, row_blocks):
    devices_all = ROWDEV * COLDEV
    starts = (jnp.cumsum(row_blocks) - row_blocks).astype(jnp.int32)
    slot_ids = jnp.arange(ROWDEV * LMAX, dtype=jnp.int32)
    usable = slot_ids % LMAX < row_blocks[slot_ids // LMAX]
    hub_now = jnp.where(usable[:, None, None], hub_seeds, jnp.zeros_like(hub_seeds))
    blocks_dev = tile_blocks.reshape(devices_all, TILE_DEV, TB, TB)
    owners = jnp.arange(devices_all, dtype=jnp.int32) // COLDEV
    rows_dev = tile_rows.reshape(devices_all, TILE_DEV)
    padded_rows = (owners[:, None] * LMAX + rows_dev - starts[owners][:, None]).astype(jnp.int32)
    cols_dev = tile_cols.reshape(devices_all, TILE_DEV)
    live_mask = (jnp.arange(TILE_DEV, dtype=jnp.int32)[None, :] < tile_count[:, None]).astype(jnp.float32)
    inputs_all = (blocks_dev, padded_rows, cols_dev, live_mask)
    authority = None
    for iteration in range(ITERS):

        def authority_step(running, inputs):
            blocks, row_ids, col_ids, weights = inputs
            picked = hub_now[row_ids].astype(jnp.float32)
            products = jnp.einsum('tkr,trc->tkc', picked, blocks.astype(jnp.float32))
            partial_value = jnp.zeros((NB, K, TB), jnp.float32).at[col_ids].add(products * weights[:, None, None])
            return (running + rounded_partial(partial_value), None)
        raw_authority, _ = lax.scan(authority_step, jnp.zeros((NB, K, TB), jnp.float32), inputs_all)
        authority = normalize(raw_authority)

        def hub_step(running, inputs):
            blocks, row_ids, col_ids, weights = inputs
            picked = authority[col_ids].astype(jnp.float32)
            products = jnp.einsum('tkc,trc->tkr', picked, blocks.astype(jnp.float32))
            partial_value = jnp.zeros((ROWDEV * LMAX, K, TB), jnp.float32).at[row_ids].add(products * weights[:, None, None])
            return (running + rounded_partial(partial_value), None)
        raw_hub, _ = lax.scan(hub_step, jnp.zeros((ROWDEV * LMAX, K, TB), jnp.float32), inputs_all)
        hub_now = normalize(raw_hub)
    return (authority, hub_now)
```

```python
import functools

import jax
import jax.numpy as jnp
from jax import lax
from jax.experimental import pallas as pl
from jax.experimental.pallas import tpu as pltpu
from jax.sharding import PartitionSpec as P

ITERS = 2
RB_DEV = 16
MESH = pl.DeviceIdType.MESH
UNROLL = 8
CHUNK = 32


def column_of(row):
    k = row.shape[1]
    eye = lax.broadcasted_iota(jnp.int32, (k, k), 0) == lax.broadcasted_iota(jnp.int32, (k, k), 1)
    return jnp.sum(jnp.where(eye, jnp.broadcast_to(row, (k, k)), 0.0), axis=1, keepdims=True)


def row_of(column, lanes):
    k = column.shape[0]
    eye = lax.broadcasted_iota(jnp.int32, (k, lanes), 0) == lax.broadcasted_iota(jnp.int32, (k, lanes), 1)
    return jnp.sum(jnp.where(eye, jnp.broadcast_to(column, (k, lanes)), 0.0), axis=0, keepdims=True)


def tiles_kernel(transposed, pick_ref, put_ref, x_ref, factor_ref, tiles_ref, out_ref, acc):
    step = pl.program_id(0)
    chunk = tiles_ref.shape[0]
    blocks = out_ref.shape[0]

    @pl.when(step == 0)
    def _():
        acc[...] = jnp.zeros_like(acc)

    dims = (((1,), (1,)), ((), ())) if transposed else (((1,), (0,)), ((), ()))

    @pl.loop(0, chunk // UNROLL)
    def _(i):
        products = []
        for u in range(UNROLL):
            t = i * UNROLL + u
            x = x_ref[pick_ref[step * chunk + t]]
            products.append(lax.dot_general(x, tiles_ref[t], dims, preferred_element_type=jnp.float32))
        for u in range(UNROLL):
            where = put_ref[step * chunk + i * UNROLL + u]
            acc[where] = acc[where] + products[u]

    @pl.when(step == pl.num_programs(0) - 1)
    def _():
        factor = factor_ref[...]

        @pl.loop(0, blocks)
        def _(b):
            out_ref[b] = (acc[b] * factor).astype(jnp.bfloat16)


def tile_sums(transposed, blocks, pick, put, x, factor, tiles):
    slots, side = tiles.shape[0], tiles.shape[1]
    k = x.shape[1]
    chunk = CHUNK
    while slots % chunk:
        chunk //= 2
    grid_spec = pltpu.PrefetchScalarGridSpec(
        num_scalar_prefetch=2,
        grid=(slots // chunk,),
        in_specs=[
            pl.BlockSpec(x.shape, lambda i, *_: (0, 0, 0)),
            pl.BlockSpec(factor.shape, lambda i, *_: (0, 0)),
            pl.BlockSpec((chunk, side, side), lambda i, *_: (i, 0, 0)),
        ],
        out_specs=pl.BlockSpec((blocks, k, side), lambda i, *_: (0, 0, 0)),
        scratch_shapes=[pltpu.VMEM((blocks + 1, k, side), jnp.float32)],
    )
    return pl.pallas_call(
        functools.partial(tiles_kernel, transposed),
        grid_spec=grid_spec,
        out_shape=jax.ShapeDtypeStruct((blocks, k, side), jnp.bfloat16),
        name="hub_tiles" if transposed else "authority_tiles",
    )(pick, put, x, factor, tiles)


def reduce_kernel(
    axis, other, n, m, g, hosts, part_ref, set_ref, factor_ref, own_ref,
    pair_in, hop_out, hop_in, own, sq_axis, sq_other,
    pair_send, pair_recv, hop_send, hop_recv,
    near_send, near_recv, far_send, far_recv,
    sqa_send, sqa_recv, sqo_send, sqo_recv,
):
    me = lax.axis_index(axis)
    mo = lax.axis_index(other)
    lo, hi = me % 2, me // 2
    highs = n // 2
    pair = hi * 2 + (1 - lo)

    def at(index):
        return {axis: index, other: mo}

    barrier = pltpu.get_barrier_semaphore()
    for d in range(1, n):
        pl.semaphore_signal(barrier, inc=1, device_id=at((me + d) % n), device_id_type=MESH)
    for d in range(1, m):
        pl.semaphore_signal(barrier, inc=1, device_id={axis: me, other: (mo + d) % m}, device_id_type=MESH)
    pl.semaphore_wait(barrier, n - 1 + m - 1)

    def group(h, l):
        return pl.ds((h * 2 + l) * g, g)

    def order(d):
        return (hi + 1 + d) % highs

    pair_copies = []
    for d in range(highs):
        h = order(d)
        copy = pltpu.make_async_remote_copy(
            src_ref=part_ref.at[group(h, 1 - lo)], dst_ref=pair_in.at[d],
            send_sem=pair_send.at[d], recv_sem=pair_recv.at[d],
            device_id=at(pair), device_id_type=MESH,
        )
        copy.start()
        pair_copies.append(copy)
    hop_copies = []
    for d in range(highs):
        h = order(d)
        pair_copies[d].wait_recv()
        total = part_ref[group(h, lo)].astype(jnp.float32) + pair_in[d].astype(jnp.float32)
        if d == highs - 1:
            own[...] = total
        else:
            hop_out[d] = total.astype(jnp.bfloat16)
            copy = pltpu.make_async_remote_copy(
                src_ref=hop_out.at[d], dst_ref=hop_in.at[d],
                send_sem=hop_send.at[d], recv_sem=hop_recv.at[d],
                device_id=at(h * 2 + lo), device_id_type=MESH,
            )
            copy.start()
            hop_copies.append(copy)
    for copy in hop_copies:
        copy.wait_recv()
    total = own[...]
    for d in range(highs - 1):
        total = total + hop_in[d].astype(jnp.float32)
    own[...] = total
    set_ref[group(hi, lo)] = total.astype(jnp.bfloat16)
    squares = jnp.sum(total * total, axis=0)
    sq_axis[me] = jnp.broadcast_to(row_of(jnp.sum(squares, axis=1, keepdims=True), 128), (8, 128))

    sqa_copies = []
    for d in range(1, n):
        copy = pltpu.make_async_remote_copy(
            src_ref=sq_axis.at[me], dst_ref=sq_axis.at[me],
            send_sem=sqa_send.at[d - 1], recv_sem=sqa_recv.at[d - 1],
            device_id=at((me + d) % n), device_id_type=MESH,
        )
        copy.start()
        sqa_copies.append(copy)
    far_copies = []
    for d in range(highs - 1):
        copy = pltpu.make_async_remote_copy(
            src_ref=set_ref.at[group(hi, lo)], dst_ref=set_ref.at[group(hi, lo)],
            send_sem=far_send.at[d], recv_sem=far_recv.at[d],
            device_id=at(order(d) * 2 + lo), device_id_type=MESH,
        )
        copy.start()
        far_copies.append(copy)

    def to_partner(d, h):
        copy = pltpu.make_async_remote_copy(
            src_ref=set_ref.at[group(h, lo)], dst_ref=set_ref.at[group(h, lo)],
            send_sem=near_send.at[d], recv_sem=near_recv.at[d],
            device_id=at(pair), device_id_type=MESH,
        )
        copy.start()
        return copy

    near_copies = [to_partner(highs - 1, hi)]

    for copy in sqa_copies:
        copy.wait_recv()
    sq_other[mo] = jnp.sum(sq_axis[...], axis=0)
    sqo_copies = []
    for d in range(1, m):
        copy = pltpu.make_async_remote_copy(
            src_ref=sq_other.at[mo], dst_ref=sq_other.at[mo],
            send_sem=sqo_send.at[d - 1], recv_sem=sqo_recv.at[d - 1],
            device_id={axis: me, other: (mo + d) % m}, device_id_type=MESH,
        )
        copy.start()
        sqo_copies.append(copy)

    for d in range(highs - 1):
        far_copies[d].wait_recv()
        near_copies.append(to_partner(d, (hi + highs - 1 - d) % highs))
    for copy in sqo_copies:
        copy.wait_recv()
    all_squares = jnp.sum(sq_other[...], axis=0)
    factor_row = 1.0 / jnp.sqrt(all_squares / hosts + 1.0)
    k = factor_ref.shape[0]
    factor = jnp.broadcast_to(column_of(factor_row[0:1, :k]), factor_ref.shape)
    factor_ref[...] = factor
    own_ref[...] = (own[...] * factor[None]).astype(jnp.bfloat16)
    for copy in near_copies:
        copy.wait_recv()
    for copy in pair_copies + hop_copies + sqa_copies + far_copies + near_copies + sqo_copies:
        copy.wait_send()


def reduce_set(axis, other, n, m, hosts, collective_id, part):
    blocks, k, side = part.shape
    g = blocks // n
    highs = n // 2
    vmem = pl.BlockSpec(memory_space=pltpu.VMEM)
    dma = lambda count: pltpu.SemaphoreType.DMA((max(count, 1),))
    return pl.pallas_call(
        functools.partial(reduce_kernel, axis, other, n, m, g, hosts),
        out_shape=(
            jax.ShapeDtypeStruct((blocks, k, side), jnp.bfloat16),
            jax.ShapeDtypeStruct((k, side), jnp.float32),
            jax.ShapeDtypeStruct((g, k, side), jnp.bfloat16),
        ),
        in_specs=[vmem],
        out_specs=(vmem, vmem, vmem),
        scratch_shapes=[
            pltpu.VMEM((highs, g, k, side), jnp.bfloat16),
            pltpu.VMEM((max(highs - 1, 1), g, k, side), jnp.bfloat16),
            pltpu.VMEM((max(highs - 1, 1), g, k, side), jnp.bfloat16),
            pltpu.VMEM((g, k, side), jnp.float32),
            pltpu.VMEM((n, 8, 128), jnp.float32),
            pltpu.VMEM((m, 8, 128), jnp.float32),
            dma(highs), dma(highs), dma(highs - 1), dma(highs - 1),
            dma(highs), dma(highs), dma(highs - 1), dma(highs - 1),
            dma(n - 1), dma(n - 1), dma(m - 1), dma(m - 1),
        ],
        compiler_params=pltpu.CompilerParams(collective_id=collective_id, has_side_effects=True),
        name="reduce_" + axis,
    )(part)


def local(row_devs, col_devs, hub_seeds, tile_blocks, tile_rows, tile_cols, tile_count, row_blocks):
    own_row = lax.axis_index("row")
    slot_count, k = hub_seeds.shape[0], hub_seeds.shape[1]
    tile_slots, tile_side = tile_blocks.shape[0], tile_blocks.shape[1]
    group_len = RB_DEV // col_devs
    set_blocks = group_len * row_devs
    host_count = RB_DEV * row_devs * tile_side
    before = jnp.arange(row_devs, dtype=jnp.int32) < own_row
    first_block = jnp.sum(jnp.where(before, row_blocks, 0))
    live = jnp.arange(tile_slots, dtype=jnp.int32) < tile_count[0]
    row_slot = tile_rows - first_block
    col_slot = tile_cols // group_len // col_devs * group_len + tile_cols % group_len
    row_pick = jnp.where(live, row_slot, 0)
    col_pick = jnp.where(live, col_slot, 0)
    row_put = jnp.where(live, row_slot, slot_count)
    col_put = jnp.where(live, col_slot, set_blocks)
    hub = hub_seeds
    factor = jnp.ones((k, tile_side), jnp.float32)
    for iteration in range(ITERS):
        part = tile_sums(False, set_blocks, row_pick, col_put, hub, factor, tile_blocks)
        column_set, factor, authority = reduce_set("row", "col", row_devs, col_devs, host_count, 0, part)
        part = tile_sums(True, slot_count, col_pick, row_put, column_set, factor, tile_blocks)
        hub, factor, _ = reduce_set("col", "row", col_devs, row_devs, host_count, 1, part)
    hub_scores = (hub.astype(jnp.float32) * factor[None]).astype(jnp.bfloat16)
    return (authority, hub_scores)


def solution(mesh):
    return jax.shard_map(
        functools.partial(local, mesh.shape["row"], mesh.shape["col"]),
        mesh=mesh,
        in_specs=(
            P("row", None, None),
            P(("row", "col"), None, None),
            P(("row", "col")),
            P(("row", "col")),
            P(("row", "col")),
            P(),
        ),
        out_specs=(P(("row", "col"), None, None), P("row", None, None)),
        check_vma=False,
    )
```

```python
import functools

import jax
import jax.numpy as jnp
from jax import lax
from jax.experimental import pallas as pl
from jax.experimental.pallas import tpu as pltpu
from jax.sharding import PartitionSpec as P

ITERS = 2
RB_DEV = 16
MESH = pl.DeviceIdType.MESH
UNROLL = 64
CHUNK = 64


def column_of(row):
    k = row.shape[1]
    eye = lax.broadcasted_iota(jnp.int32, (k, k), 0) == lax.broadcasted_iota(jnp.int32, (k, k), 1)
    return jnp.sum(jnp.where(eye, jnp.broadcast_to(row, (k, k)), 0.0), axis=1, keepdims=True)


def row_of(column, lanes):
    k = column.shape[0]
    eye = lax.broadcasted_iota(jnp.int32, (k, lanes), 0) == lax.broadcasted_iota(jnp.int32, (k, lanes), 1)
    return jnp.sum(jnp.where(eye, jnp.broadcast_to(column, (k, lanes)), 0.0), axis=0, keepdims=True)


def tiles_kernel(transposed, pick_ref, put_ref, x_ref, tiles_ref, out_ref, acc):
    step = pl.program_id(0)
    chunk = tiles_ref.shape[0]
    blocks = out_ref.shape[0]

    @pl.when(step == 0)
    def _():
        acc[...] = jnp.zeros_like(acc)

    dims = (((1,), (1,)), ((), ())) if transposed else (((1,), (0,)), ((), ()))

    side = tiles_ref.shape[1]
    k = x_ref.shape[1]

    @pl.loop(0, chunk // UNROLL)
    def _(i):
        products = []
        for u in range(0, UNROLL, 2):
            t = i * UNROLL + u
            x = jnp.concatenate([x_ref[pick_ref[step * chunk + t + v]] for v in range(2)], axis=0)
            if transposed:
                both = tiles_ref[pl.ds(t, 2)].reshape(2 * side, side)
            else:
                both = jnp.concatenate([tiles_ref[t], tiles_ref[t + 1]], axis=1)
            product = lax.dot_general(x, both, dims, preferred_element_type=jnp.float32)
            products += [product[:k, :side], product[k:, side:]]
        for u in range(UNROLL):
            where = put_ref[step * chunk + i * UNROLL + u]
            acc[where] = acc[where] + products[u]

    @pl.when(step == pl.num_programs(0) - 1)
    def _():
        @pl.loop(0, blocks)
        def _(b):
            out_ref[b] = acc[b].astype(jnp.bfloat16)


def tile_sums(transposed, blocks, pick, put, x, tiles):
    slots, side = tiles.shape[0], tiles.shape[1]
    k = x.shape[1]
    chunk = CHUNK
    while slots % chunk:
        chunk //= 2
    grid_spec = pltpu.PrefetchScalarGridSpec(
        num_scalar_prefetch=2,
        grid=(slots // chunk,),
        in_specs=[
            pl.BlockSpec(x.shape, lambda i, *_: (0, 0, 0)),
            pl.BlockSpec((chunk, side, side), lambda i, *_: (i, 0, 0)),
        ],
        out_specs=pl.BlockSpec((blocks, k, side), lambda i, *_: (0, 0, 0)),
        scratch_shapes=[pltpu.VMEM((blocks + 1, k, side), jnp.float32)],
    )
    return pl.pallas_call(
        functools.partial(tiles_kernel, transposed),
        grid_spec=grid_spec,
        out_shape=jax.ShapeDtypeStruct((blocks, k, side), jnp.bfloat16),
        name="hub_tiles" if transposed else "authority_tiles",
    )(pick, put, x, tiles)


def factor_of(squares, hosts, k, side):
    row = 1.0 / jnp.sqrt(squares / hosts + 1.0)
    return jnp.broadcast_to(column_of(row[0:1, :k]), (k, side))


def reduce_kernel(axis, other, n, m, g, hosts, scaled, final, *refs):
    refs = list(refs)
    part_ref = refs.pop(0)
    sq_ref = refs.pop(0) if scaled else None
    set_ref = refs.pop(0)
    if final:
        before_ref, after_ref = refs.pop(0), refs.pop(0)
    else:
        sq_out_ref, own = refs.pop(0), refs.pop(0)
    pair_in, hop_out, hop_in, sq_before, sq_axis, sq_other = refs[:6]
    refs = refs[6:]
    if final:
        own = refs.pop(0)
    (pair_send, pair_recv, hop_send, hop_recv, near_send, near_recv, far_send, far_recv,
     sqb_send, sqb_recv, sqa_send, sqa_recv, sqo_send, sqo_recv) = refs
    k, side = part_ref.shape[1], part_ref.shape[2]
    me = lax.axis_index(axis)
    mo = lax.axis_index(other)
    lo, hi = me % 2, me // 2
    highs = n // 2
    pair = hi * 2 + (1 - lo)
    waits = []

    def at(index):
        return {axis: index, other: mo}

    def send(src, dst, send_sem, recv_sem, device):
        copy = pltpu.make_async_remote_copy(
            src_ref=src, dst_ref=dst, send_sem=send_sem, recv_sem=recv_sem,
            device_id=device, device_id_type=MESH,
        )
        copy.start()
        waits.append(copy)
        return copy

    barrier = pltpu.get_barrier_semaphore()
    for d in range(1, n):
        pl.semaphore_signal(barrier, inc=1, device_id=at((me + d) % n), device_id_type=MESH)
    if final:
        for d in range(1, m):
            pl.semaphore_signal(barrier, inc=1, device_id={axis: me, other: (mo + d) % m}, device_id_type=MESH)
    pl.semaphore_wait(barrier, n - 1 + (m - 1 if final else 0))

    def group(h, l):
        return pl.ds((h * 2 + l) * g, g)

    def order(d):
        return (hi + 1 + d) % highs

    pair_copies = [
        send(part_ref.at[group(order(d), 1 - lo)], pair_in.at[d], pair_send.at[d], pair_recv.at[d], at(pair))
        for d in range(highs)
    ]
    sqb_copies = []
    if scaled:
        sq_before[me] = sq_ref[...]
        sqb_copies = [
            send(sq_ref, sq_before.at[me], sqb_send.at[d - 1], sqb_recv.at[d - 1], at((me + d) % n))
            for d in range(1, n)
        ]
    hop_copies = []
    for d in range(highs):
        h = order(d)
        pair_copies[d].wait_recv()
        total = part_ref[group(h, lo)].astype(jnp.float32) + pair_in[d].astype(jnp.float32)
        if d == highs - 1:
            own[...] = total
        else:
            hop_out[d] = total.astype(jnp.bfloat16)
            hop_copies.append(send(hop_out.at[d], hop_in.at[d], hop_send.at[d], hop_recv.at[d], at(h * 2 + lo)))
    if scaled:
        for copy in sqb_copies:
            copy.wait_recv()
        factor = factor_of(jnp.sum(sq_before[...], axis=0), hosts, k, side)
        if final:
            before_ref[...] = factor
    for copy in hop_copies:
        copy.wait_recv()
    total = own[...]
    for d in range(highs - 1):
        total = total + hop_in[d].astype(jnp.float32)
    if scaled:
        total = total * factor[None]
    own[...] = total
    set_ref[group(hi, lo)] = total.astype(jnp.bfloat16)

    far_copies = [
        send(set_ref.at[group(hi, lo)], set_ref.at[group(hi, lo)], far_send.at[d], far_recv.at[d], at(order(d) * 2 + lo))
        for d in range(highs - 1)
    ]

    def to_partner(d, h):
        return send(set_ref.at[group(h, lo)], set_ref.at[group(h, lo)], near_send.at[d], near_recv.at[d], at(pair))

    near_copies = [to_partner(highs - 1, hi)]
    squares = jnp.sum(total * total, axis=0)
    sq_axis[me] = jnp.broadcast_to(row_of(jnp.sum(squares, axis=1, keepdims=True), 128), (8, 128))
    sqa_copies = [
        send(sq_axis.at[me], sq_axis.at[me], sqa_send.at[d - 1], sqa_recv.at[d - 1], at((me + d) % n))
        for d in range(1, n)
    ]

    def axis_squares():
        for copy in sqa_copies:
            copy.wait_recv()
        return jnp.sum(sq_axis[...], axis=0)

    sqo_copies = []
    if final:
        sq_other[mo] = axis_squares()
        sqo_copies = [
            send(sq_other.at[mo], sq_other.at[mo], sqo_send.at[d - 1], sqo_recv.at[d - 1], {axis: me, other: (mo + d) % m})
            for d in range(1, m)
        ]
    for d in range(highs - 1):
        far_copies[d].wait_recv()
        near_copies.append(to_partner(d, (hi + highs - 1 - d) % highs))
    if final:
        for copy in sqo_copies:
            copy.wait_recv()
        after_ref[...] = factor_of(jnp.sum(sq_other[...], axis=0), hosts, k, side)
    else:
        sq_out_ref[...] = axis_squares()
    for copy in near_copies:
        copy.wait_recv()
    for copy in waits:
        copy.wait_send()


def reduce_set(axis, other, n, m, hosts, collective_id, final, part, squares=None):
    blocks, k, side = part.shape
    g = blocks // n
    highs = n // 2
    vmem = pl.BlockSpec(memory_space=pltpu.VMEM)
    dma = lambda count: pltpu.SemaphoreType.DMA((max(count, 1),))
    scaled = squares is not None
    table = jax.ShapeDtypeStruct((k, side), jnp.float32)
    outs = [jax.ShapeDtypeStruct((blocks, k, side), jnp.bfloat16)]
    scratch = []
    if final:
        outs += [table, table]
        scratch = [pltpu.VMEM((g, k, side), jnp.float32)]
    else:
        outs += [jax.ShapeDtypeStruct((8, 128), jnp.float32), jax.ShapeDtypeStruct((g, k, side), jnp.float32)]
    operands = (part, squares) if scaled else (part,)
    return pl.pallas_call(
        functools.partial(reduce_kernel, axis, other, n, m, g, hosts, scaled, final),
        out_shape=tuple(outs),
        in_specs=[vmem] * len(operands),
        out_specs=(vmem,) * len(outs),
        scratch_shapes=[
            pltpu.VMEM((highs, g, k, side), jnp.bfloat16),
            pltpu.VMEM((max(highs - 1, 1), g, k, side), jnp.bfloat16),
            pltpu.VMEM((max(highs - 1, 1), g, k, side), jnp.bfloat16),
            pltpu.VMEM((n, 8, 128), jnp.float32),
            pltpu.VMEM((n, 8, 128), jnp.float32),
            pltpu.VMEM((m, 8, 128), jnp.float32),
            *scratch,
            dma(highs), dma(highs), dma(highs - 1), dma(highs - 1),
            dma(highs), dma(highs), dma(highs - 1), dma(highs - 1),
            dma(n - 1), dma(n - 1), dma(n - 1), dma(n - 1), dma(m - 1), dma(m - 1),
        ],
        compiler_params=pltpu.CompilerParams(collective_id=collective_id, has_side_effects=True),
        name="reduce_" + axis,
    )(*operands)


def local(row_devs, col_devs, hub_seeds, tile_blocks, tile_rows, tile_cols, tile_count, row_blocks):
    own_row = lax.axis_index("row")
    slot_count = hub_seeds.shape[0]
    tile_slots, tile_side = tile_blocks.shape[0], tile_blocks.shape[1]
    group_len = RB_DEV // col_devs
    set_blocks = group_len * row_devs
    host_count = RB_DEV * row_devs * tile_side
    first_block = jnp.zeros((1,), jnp.int32)
    for r in range(row_devs - 1):
        first_block = first_block + jnp.where(own_row > r, row_blocks[r:r + 1], 0)
    live = jnp.arange(tile_slots, dtype=jnp.int32) < tile_count
    row_slot = tile_rows - first_block
    col_slot = tile_cols // group_len // col_devs * group_len + tile_cols % group_len
    row_pick = jnp.where(live, row_slot, 0)
    col_pick = jnp.where(live, col_slot, 0)
    row_put = jnp.where(live, row_slot, slot_count)
    col_put = jnp.where(live, col_slot, set_blocks)
    hub, squares = hub_seeds, None
    for iteration in range(ITERS):
        last = iteration == ITERS - 1
        part = tile_sums(False, set_blocks, row_pick, col_put, hub, tile_blocks)
        column_set, squares, own = reduce_set(
            "row", "col", row_devs, col_devs, host_count, iteration, False, part, squares)
        part = tile_sums(True, slot_count, col_pick, row_put, column_set, tile_blocks)
        hub, squares, rest = reduce_set(
            "col", "row", col_devs, row_devs, host_count, ITERS + iteration, last, part, squares)
    authority = (own * squares[None]).astype(jnp.bfloat16)
    hub_scores = (hub.astype(jnp.float32) * rest[None]).astype(jnp.bfloat16)
    return (authority, hub_scores)


def solution(mesh):
    return jax.shard_map(
        functools.partial(local, mesh.shape["row"], mesh.shape["col"]),
        mesh=mesh,
        in_specs=(
            P("row", None, None),
            P(("row", "col"), None, None),
            P(("row", "col")),
            P(("row", "col")),
            P(("row", "col")),
            P(),
        ),
        out_specs=(P(("row", "col"), None, None), P("row", None, None)),
        check_vma=False,
    )
```

```python
import functools

import jax
import jax.numpy as jnp
from jax import lax
from jax.experimental import pallas as pl
from jax.experimental.pallas import tpu as pltpu
from jax.sharding import PartitionSpec as P

ITERS = 2
RB_DEV = 16
MESH = pl.DeviceIdType.MESH
UNROLL = 128
CHUNK = 128


def column_of(row):
    k = row.shape[1]
    eye = lax.broadcasted_iota(jnp.int32, (k, k), 0) == lax.broadcasted_iota(jnp.int32, (k, k), 1)
    return jnp.sum(jnp.where(eye, jnp.broadcast_to(row, (k, k)), 0.0), axis=1, keepdims=True)


def row_of(column, lanes):
    k = column.shape[0]
    eye = lax.broadcasted_iota(jnp.int32, (k, lanes), 0) == lax.broadcasted_iota(jnp.int32, (k, lanes), 1)
    return jnp.sum(jnp.where(eye, jnp.broadcast_to(column, (k, lanes)), 0.0), axis=0, keepdims=True)


def tiles_kernel(transposed, pick_ref, put_ref, x_ref, tiles_ref, out_ref, acc):
    step = pl.program_id(0)
    chunk = tiles_ref.shape[0]
    blocks = out_ref.shape[0]

    @pl.when(step == 0)
    def _():
        acc[...] = jnp.zeros_like(acc)

    dims = (((1,), (1,)), ((), ())) if transposed else (((1,), (0,)), ((), ()))

    side = tiles_ref.shape[1]
    k = x_ref.shape[1]

    @pl.loop(0, chunk // UNROLL)
    def _(i):
        products = []
        for u in range(0, UNROLL, 2):
            t = i * UNROLL + u
            x = jnp.concatenate([x_ref[pick_ref[step * chunk + t + v]] for v in range(2)], axis=0)
            if transposed:
                both = tiles_ref[pl.ds(t, 2)].reshape(2 * side, side)
            else:
                both = jnp.concatenate([tiles_ref[t], tiles_ref[t + 1]], axis=1)
            product = lax.dot_general(x, both, dims, preferred_element_type=jnp.float32)
            products += [product[:k, :side], product[k:, side:]]
        for u in range(UNROLL):
            where = put_ref[step * chunk + i * UNROLL + u]
            acc[where] = acc[where] + products[u]

    @pl.when(step == pl.num_programs(0) - 1)
    def _():
        @pl.loop(0, blocks)
        def _(b):
            out_ref[b] = acc[b].astype(jnp.bfloat16)


def tile_sums(transposed, blocks, pick, put, x, tiles):
    slots, side = tiles.shape[0], tiles.shape[1]
    k = x.shape[1]
    chunk = CHUNK
    while slots % chunk:
        chunk //= 2
    grid_spec = pltpu.PrefetchScalarGridSpec(
        num_scalar_prefetch=2,
        grid=(slots // chunk,),
        in_specs=[
            pl.BlockSpec(x.shape, lambda i, *_: (0, 0, 0)),
            pl.BlockSpec((chunk, side, side), lambda i, *_: (i, 0, 0)),
        ],
        out_specs=pl.BlockSpec((blocks, k, side), lambda i, *_: (0, 0, 0)),
        scratch_shapes=[pltpu.VMEM((blocks + 1, k, side), jnp.float32)],
    )
    return pl.pallas_call(
        functools.partial(tiles_kernel, transposed),
        grid_spec=grid_spec,
        out_shape=jax.ShapeDtypeStruct((blocks, k, side), jnp.bfloat16),
        name="hub_tiles" if transposed else "authority_tiles",
    )(pick, put, x, tiles)


def factor_of(squares, hosts, k, side):
    row = 1.0 / jnp.sqrt(squares / hosts + 1.0)
    return jnp.broadcast_to(column_of(row[0:1, :k]), (k, side))


def reduce_kernel(axis, other, n, m, g, hosts, scaled, final, *refs):
    refs = list(refs)
    part_ref = refs.pop(0)
    sq_ref = refs.pop(0) if scaled else None
    set_ref = refs.pop(0)
    if final:
        before_ref, after_ref = refs.pop(0), refs.pop(0)
    else:
        sq_out_ref, own = refs.pop(0), refs.pop(0)
    pair_in, hop_out, hop_in, sq_before, sq_axis, sq_other = refs[:6]
    refs = refs[6:]
    if final:
        own = refs.pop(0)
    (pair_send, pair_recv, hop_send, hop_recv, near_send, near_recv, far_send, far_recv,
     sqb_send, sqb_recv, sqa_send, sqa_recv, sqo_send, sqo_recv) = refs
    k, side = part_ref.shape[1], part_ref.shape[2]
    me = lax.axis_index(axis)
    mo = lax.axis_index(other)
    lo, hi = me % 2, me // 2
    highs = n // 2
    pair = hi * 2 + (1 - lo)
    waits = []

    def at(index):
        return {axis: index, other: mo}

    def send(src, dst, send_sem, recv_sem, device):
        copy = pltpu.make_async_remote_copy(
            src_ref=src, dst_ref=dst, send_sem=send_sem, recv_sem=recv_sem,
            device_id=device, device_id_type=MESH,
        )
        copy.start()
        waits.append(copy)
        return copy

    barrier = pltpu.get_barrier_semaphore()
    for d in range(1, n):
        pl.semaphore_signal(barrier, inc=1, device_id=at((me + d) % n), device_id_type=MESH)
    if final:
        for d in range(1, m):
            pl.semaphore_signal(barrier, inc=1, device_id={axis: me, other: (mo + d) % m}, device_id_type=MESH)
    pl.semaphore_wait(barrier, n - 1 + (m - 1 if final else 0))

    def group(h, l):
        return pl.ds((h * 2 + l) * g, g)

    def order(d):
        return (hi + 1 + d) % highs

    pair_copies = [
        send(part_ref.at[group(order(d), 1 - lo)], pair_in.at[d], pair_send.at[d], pair_recv.at[d], at(pair))
        for d in range(highs)
    ]
    sqb_copies = []
    if scaled:
        sq_before[me] = sq_ref[...]
        sqb_copies = [
            send(sq_ref, sq_before.at[me], sqb_send.at[d - 1], sqb_recv.at[d - 1], at((me + d) % n))
            for d in range(1, n)
        ]
    hop_copies = []
    for d in range(highs):
        h = order(d)
        pair_copies[d].wait_recv()
        total = part_ref[group(h, lo)].astype(jnp.float32) + pair_in[d].astype(jnp.float32)
        if d == highs - 1:
            own[...] = total
        else:
            hop_out[d] = total.astype(jnp.bfloat16)
            hop_copies.append(send(hop_out.at[d], hop_in.at[d], hop_send.at[d], hop_recv.at[d], at(h * 2 + lo)))
    if scaled:
        for copy in sqb_copies:
            copy.wait_recv()
        factor = factor_of(jnp.sum(sq_before[...], axis=0), hosts, k, side)
        if final:
            before_ref[...] = factor
    for copy in hop_copies:
        copy.wait_recv()
    total = own[...]
    for d in range(highs - 1):
        total = total + hop_in[d].astype(jnp.float32)
    if scaled:
        total = total * factor[None]
    own[...] = total
    set_ref[group(hi, lo)] = total.astype(jnp.bfloat16)

    def send_squares():
        squares = jnp.sum(total * total, axis=0)
        sq_axis[me] = jnp.broadcast_to(row_of(jnp.sum(squares, axis=1, keepdims=True), 128), (8, 128))
        return [
            send(sq_axis.at[me], sq_axis.at[me], sqa_send.at[d - 1], sqa_recv.at[d - 1], at((me + d) % n))
            for d in range(1, n)
        ]

    if final:
        sqa_copies = send_squares()
    far_copies = [
        send(set_ref.at[group(hi, lo)], set_ref.at[group(hi, lo)], far_send.at[d], far_recv.at[d], at(order(d) * 2 + lo))
        for d in range(highs - 1)
    ]

    def to_partner(d, h):
        return send(set_ref.at[group(h, lo)], set_ref.at[group(h, lo)], near_send.at[d], near_recv.at[d], at(pair))

    near_copies = [to_partner(highs - 1, hi)]
    if not final:
        sqa_copies = send_squares()

    def axis_squares():
        for copy in sqa_copies:
            copy.wait_recv()
        return jnp.sum(sq_axis[...], axis=0)

    sqo_copies = []
    if final:
        sq_other[mo] = axis_squares()
        sqo_copies = [
            send(sq_other.at[mo], sq_other.at[mo], sqo_send.at[d - 1], sqo_recv.at[d - 1], {axis: me, other: (mo + d) % m})
            for d in range(1, m)
        ]
    for d in range(highs - 1):
        far_copies[d].wait_recv()
        near_copies.append(to_partner(d, (hi + highs - 1 - d) % highs))
    if final:
        for copy in sqo_copies:
            copy.wait_recv()
        after_ref[...] = factor_of(jnp.sum(sq_other[...], axis=0), hosts, k, side)
    else:
        sq_out_ref[...] = axis_squares()
    for copy in near_copies:
        copy.wait_recv()
    for copy in waits:
        copy.wait_send()


def reduce_set(axis, other, n, m, hosts, collective_id, final, part, squares=None):
    blocks, k, side = part.shape
    g = blocks // n
    highs = n // 2
    vmem = pl.BlockSpec(memory_space=pltpu.VMEM)
    dma = lambda count: pltpu.SemaphoreType.DMA((max(count, 1),))
    scaled = squares is not None
    table = jax.ShapeDtypeStruct((k, side), jnp.float32)
    outs = [jax.ShapeDtypeStruct((blocks, k, side), jnp.bfloat16)]
    scratch = []
    if final:
        outs += [table, table]
        scratch = [pltpu.VMEM((g, k, side), jnp.float32)]
    else:
        outs += [jax.ShapeDtypeStruct((8, 128), jnp.float32), jax.ShapeDtypeStruct((g, k, side), jnp.float32)]
    operands = (part, squares) if scaled else (part,)
    return pl.pallas_call(
        functools.partial(reduce_kernel, axis, other, n, m, g, hosts, scaled, final),
        out_shape=tuple(outs),
        in_specs=[vmem] * len(operands),
        out_specs=(vmem,) * len(outs),
        scratch_shapes=[
            pltpu.VMEM((highs, g, k, side), jnp.bfloat16),
            pltpu.VMEM((max(highs - 1, 1), g, k, side), jnp.bfloat16),
            pltpu.VMEM((max(highs - 1, 1), g, k, side), jnp.bfloat16),
            pltpu.VMEM((n, 8, 128), jnp.float32),
            pltpu.VMEM((n, 8, 128), jnp.float32),
            pltpu.VMEM((m, 8, 128), jnp.float32),
            *scratch,
            dma(highs), dma(highs), dma(highs - 1), dma(highs - 1),
            dma(highs), dma(highs), dma(highs - 1), dma(highs - 1),
            dma(n - 1), dma(n - 1), dma(n - 1), dma(n - 1), dma(m - 1), dma(m - 1),
        ],
        compiler_params=pltpu.CompilerParams(collective_id=collective_id, has_side_effects=True),
        name="reduce_" + axis,
    )(*operands)


def local(row_devs, col_devs, hub_seeds, tile_blocks, tile_rows, tile_cols, tile_count, row_blocks):
    own_row = lax.axis_index("row")
    slot_count = hub_seeds.shape[0]
    tile_slots, tile_side = tile_blocks.shape[0], tile_blocks.shape[1]
    group_len = RB_DEV // col_devs
    set_blocks = group_len * row_devs
    host_count = RB_DEV * row_devs * tile_side
    before = jnp.arange(row_devs, dtype=jnp.int32) < own_row
    first_block = jnp.sum(jnp.where(before, row_blocks, 0))
    live = jnp.arange(tile_slots, dtype=jnp.int32) < tile_count[0]
    row_slot = tile_rows - first_block
    col_slot = tile_cols // group_len // col_devs * group_len + tile_cols % group_len
    row_pick = jnp.where(live, row_slot, 0)
    col_pick = jnp.where(live, col_slot, 0)
    row_put = jnp.where(live, row_slot, slot_count)
    col_put = jnp.where(live, col_slot, set_blocks)
    hub, squares = hub_seeds, None
    for iteration in range(ITERS):
        last = iteration == ITERS - 1
        part = tile_sums(False, set_blocks, row_pick, col_put, hub, tile_blocks)
        column_set, squares, own = reduce_set(
            "row", "col", row_devs, col_devs, host_count, iteration, False, part, squares)
        part = tile_sums(True, slot_count, col_pick, row_put, column_set, tile_blocks)
        hub, squares, rest = reduce_set(
            "col", "row", col_devs, row_devs, host_count, ITERS + iteration, last, part, squares)
    authority = (own * squares[None]).astype(jnp.bfloat16)
    hub_scores = (hub.astype(jnp.float32) * rest[None]).astype(jnp.bfloat16)
    return (authority, hub_scores)


def solution(mesh):
    return jax.shard_map(
        functools.partial(local, mesh.shape["row"], mesh.shape["col"]),
        mesh=mesh,
        in_specs=(
            P("row", None, None),
            P(("row", "col"), None, None),
            P(("row", "col")),
            P(("row", "col")),
            P(("row", "col")),
            P(),
        ),
        out_specs=(P(("row", "col"), None, None), P("row", None, None)),
        check_vma=False,
    )
```

```python
import functools

import jax
import jax.numpy as jnp
from jax import lax
from jax.experimental import pallas as pl
from jax.experimental.pallas import tpu as pltpu
from jax.sharding import PartitionSpec as P

ITERS = 2
RB_DEV = 16
MESH = pl.DeviceIdType.MESH
MIB = 1 << 20
UNROLL = 128
LIMIT_MIB = 4


def column_of(row):
    k = row.shape[1]
    eye = lax.broadcasted_iota(jnp.int32, (k, k), 0) == lax.broadcasted_iota(jnp.int32, (k, k), 1)
    return jnp.sum(jnp.where(eye, jnp.broadcast_to(row, (k, k)), 0.0), axis=1, keepdims=True)


def row_of(column, lanes):
    k = column.shape[0]
    eye = lax.broadcasted_iota(jnp.int32, (k, lanes), 0) == lax.broadcasted_iota(jnp.int32, (k, lanes), 1)
    return jnp.sum(jnp.where(eye, jnp.broadcast_to(column, (k, lanes)), 0.0), axis=0, keepdims=True)


def tiles_kernel(transposed, pick_ref, put_ref, x_ref, tiles_ref, out_ref, acc):
    step = pl.program_id(0)
    chunk = UNROLL
    blocks = out_ref.shape[0]
    side, k = tiles_ref.shape[1], x_ref.shape[1]
    base = 0 if tiles_ref.shape[0] == chunk else step * chunk

    @pl.when(step == 0)
    def _():
        acc[...] = jnp.zeros_like(acc)

    dims = (((1,), (1,)), ((), ())) if transposed else (((1,), (0,)), ((), ()))

    products = []
    for u in range(0, chunk, 2):
        x = jnp.concatenate([x_ref[pick_ref[step * chunk + u + v]] for v in range(2)], axis=0)
        if transposed:
            both = tiles_ref[pl.ds(base + u, 2)].reshape(2 * side, side)
        else:
            both = jnp.concatenate([tiles_ref[base + u], tiles_ref[base + u + 1]], axis=1)
        product = lax.dot_general(x, both, dims, preferred_element_type=jnp.float32)
        products += [product[:k, :side], product[k:, side:]]
    for u in range(chunk):
        where = put_ref[step * chunk + u]
        acc[where] = acc[where] + products[u]

    @pl.when(step == pl.num_programs(0) - 1)
    def _():
        @pl.loop(0, blocks)
        def _(b):
            out_ref[b] = acc[b].astype(jnp.bfloat16)


def tile_sums(transposed, blocks, pick, put, x, tiles, resident):
    slots, side = tiles.shape[0], tiles.shape[1]
    k = x.shape[1]
    vmem = pl.BlockSpec(memory_space=pltpu.VMEM)
    held = 2 * UNROLL * side * side * 2
    streamed = pl.BlockSpec((UNROLL, side, side), lambda i, *_: (i, 0, 0))
    grid_spec = pltpu.PrefetchScalarGridSpec(
        num_scalar_prefetch=2,
        grid=(slots // UNROLL,),
        in_specs=[vmem, vmem if resident else streamed],
        out_specs=vmem,
        scratch_shapes=[pltpu.VMEM((blocks + 1, k, side), jnp.float32)],
    )
    return pl.pallas_call(
        functools.partial(tiles_kernel, transposed),
        grid_spec=grid_spec,
        out_shape=jax.ShapeDtypeStruct((blocks, k, side), jnp.bfloat16),
        compiler_params=pltpu.CompilerParams(
            vmem_limit_bytes=(0 if resident else held) + (x.size + blocks * k * side * 3) * 2 + LIMIT_MIB * MIB),
        name="hub_tiles" if transposed else "authority_tiles",
    )(pick, put, x, tiles)


def factor_of(squares, hosts, k, side):
    row = 1.0 / jnp.sqrt(squares / hosts + 1.0)
    return jnp.broadcast_to(column_of(row[0:1, :k]), (k, side))


def reduce_kernel(axis, other, n, m, g, hosts, scaled, final, *refs):
    refs = list(refs)
    part_ref = refs.pop(0)
    sq_ref = refs.pop(0) if scaled else None
    set_ref = refs.pop(0)
    if final:
        before_ref, after_ref = refs.pop(0), refs.pop(0)
    else:
        sq_out_ref, own = refs.pop(0), refs.pop(0)
    pair_in, hop_out, hop_in, sq_before, sq_axis, sq_other = refs[:6]
    refs = refs[6:]
    if final:
        own = refs.pop(0)
    (pair_send, pair_recv, hop_send, hop_recv, near_send, near_recv, far_send, far_recv,
     sqb_send, sqb_recv, sqa_send, sqa_recv, sqo_send, sqo_recv) = refs
    k, side = part_ref.shape[1], part_ref.shape[2]
    me = lax.axis_index(axis)
    mo = lax.axis_index(other)
    lo, hi = me % 2, me // 2
    highs = n // 2
    pair = hi * 2 + (1 - lo)
    waits = []

    def at(index):
        return {axis: index, other: mo}

    def send(src, dst, send_sem, recv_sem, device):
        copy = pltpu.make_async_remote_copy(
            src_ref=src, dst_ref=dst, send_sem=send_sem, recv_sem=recv_sem,
            device_id=device, device_id_type=MESH,
        )
        copy.start()
        waits.append(copy)
        return copy

    barrier = pltpu.get_barrier_semaphore()
    for d in range(1, n):
        pl.semaphore_signal(barrier, inc=1, device_id=at((me + d) % n), device_id_type=MESH)
    if final:
        for d in range(1, m):
            pl.semaphore_signal(barrier, inc=1, device_id={axis: me, other: (mo + d) % m}, device_id_type=MESH)
    pl.semaphore_wait(barrier, n - 1 + (m - 1 if final else 0))

    def group(h, l):
        return pl.ds((h * 2 + l) * g, g)

    def order(d):
        return (hi + 1 + d) % highs

    pair_copies = [
        send(part_ref.at[group(order(d), 1 - lo)], pair_in.at[d], pair_send.at[d], pair_recv.at[d], at(pair))
        for d in range(highs)
    ]
    sqb_copies = []
    if scaled:
        sq_before[me] = sq_ref[...]
        sqb_copies = [
            send(sq_ref, sq_before.at[me], sqb_send.at[d - 1], sqb_recv.at[d - 1], at((me + d) % n))
            for d in range(1, n)
        ]
    hop_copies = []
    for d in range(highs):
        h = order(d)
        pair_copies[d].wait_recv()
        total = part_ref[group(h, lo)].astype(jnp.float32) + pair_in[d].astype(jnp.float32)
        if d == highs - 1:
            own[...] = total
        else:
            hop_out[d] = total.astype(jnp.bfloat16)
            hop_copies.append(send(hop_out.at[d], hop_in.at[d], hop_send.at[d], hop_recv.at[d], at(h * 2 + lo)))
    if scaled:
        for copy in sqb_copies:
            copy.wait_recv()
        factor = factor_of(jnp.sum(sq_before[...], axis=0), hosts, k, side)
        if final:
            before_ref[...] = factor
    for copy in hop_copies:
        copy.wait_recv()
    total = own[...]
    for d in range(highs - 1):
        total = total + hop_in[d].astype(jnp.float32)
    if scaled:
        total = total * factor[None]
    own[...] = total
    set_ref[group(hi, lo)] = total.astype(jnp.bfloat16)

    def send_squares():
        squares = jnp.sum(total * total, axis=0)
        sq_axis[me] = jnp.broadcast_to(row_of(jnp.sum(squares, axis=1, keepdims=True), 128), (8, 128))
        return [
            send(sq_axis.at[me], sq_axis.at[me], sqa_send.at[d - 1], sqa_recv.at[d - 1], at((me + d) % n))
            for d in range(1, n)
        ]

    if final:
        sqa_copies = send_squares()
    far_copies = [
        send(set_ref.at[group(hi, lo)], set_ref.at[group(hi, lo)], far_send.at[d], far_recv.at[d], at(order(d) * 2 + lo))
        for d in range(highs - 1)
    ]

    def to_partner(d, h):
        return send(set_ref.at[group(h, lo)], set_ref.at[group(h, lo)], near_send.at[d], near_recv.at[d], at(pair))

    near_copies = [to_partner(highs - 1, hi)]
    if not final:
        sqa_copies = send_squares()

    def axis_squares():
        for copy in sqa_copies:
            copy.wait_recv()
        return jnp.sum(sq_axis[...], axis=0)

    sqo_copies = []
    if final:
        sq_other[mo] = axis_squares()
        sqo_copies = [
            send(sq_other.at[mo], sq_other.at[mo], sqo_send.at[d - 1], sqo_recv.at[d - 1], {axis: me, other: (mo + d) % m})
            for d in range(1, m)
        ]
    for d in range(highs - 1):
        far_copies[d].wait_recv()
        near_copies.append(to_partner(d, (hi + highs - 1 - d) % highs))
    if final:
        for copy in sqo_copies:
            copy.wait_recv()
        after_ref[...] = factor_of(jnp.sum(sq_other[...], axis=0), hosts, k, side)
    else:
        sq_out_ref[...] = axis_squares()
    for copy in near_copies:
        copy.wait_recv()
    for copy in waits:
        copy.wait_send()


def reduce_set(axis, other, n, m, hosts, collective_id, final, part, squares=None):
    blocks, k, side = part.shape
    g = blocks // n
    highs = n // 2
    vmem = pl.BlockSpec(memory_space=pltpu.VMEM)
    dma = lambda count: pltpu.SemaphoreType.DMA((max(count, 1),))
    scaled = squares is not None
    table = jax.ShapeDtypeStruct((k, side), jnp.float32)
    outs = [jax.ShapeDtypeStruct((blocks, k, side), jnp.bfloat16)]
    scratch = []
    if final:
        outs += [table, table]
        scratch = [pltpu.VMEM((g, k, side), jnp.float32)]
    else:
        outs += [jax.ShapeDtypeStruct((8, 128), jnp.float32), jax.ShapeDtypeStruct((g, k, side), jnp.float32)]
    operands = (part, squares) if scaled else (part,)
    return pl.pallas_call(
        functools.partial(reduce_kernel, axis, other, n, m, g, hosts, scaled, final),
        out_shape=tuple(outs),
        in_specs=[vmem] * len(operands),
        out_specs=(vmem,) * len(outs),
        scratch_shapes=[
            pltpu.VMEM((highs, g, k, side), jnp.bfloat16),
            pltpu.VMEM((max(highs - 1, 1), g, k, side), jnp.bfloat16),
            pltpu.VMEM((max(highs - 1, 1), g, k, side), jnp.bfloat16),
            pltpu.VMEM((n, 8, 128), jnp.float32),
            pltpu.VMEM((n, 8, 128), jnp.float32),
            pltpu.VMEM((m, 8, 128), jnp.float32),
            *scratch,
            dma(highs), dma(highs), dma(highs - 1), dma(highs - 1),
            dma(highs), dma(highs), dma(highs - 1), dma(highs - 1),
            dma(n - 1), dma(n - 1), dma(n - 1), dma(n - 1), dma(m - 1), dma(m - 1),
        ],
        compiler_params=pltpu.CompilerParams(
            collective_id=collective_id, has_side_effects=True, vmem_limit_bytes=6 * part.size * 2 + 4 * MIB),
        name="reduce_" + axis,
    )(*operands)


def local(row_devs, col_devs, hub_seeds, tile_blocks, tile_rows, tile_cols, tile_count, row_blocks):
    own_row = lax.axis_index("row")
    slot_count = hub_seeds.shape[0]
    tile_slots, tile_side = tile_blocks.shape[0], tile_blocks.shape[1]
    group_len = RB_DEV // col_devs
    set_blocks = group_len * row_devs
    host_count = RB_DEV * row_devs * tile_side
    before = jnp.arange(row_devs, dtype=jnp.int32) < own_row
    first_block = jnp.sum(jnp.where(before, row_blocks, 0))
    live = jnp.arange(tile_slots, dtype=jnp.int32) < tile_count[0]
    row_slot = tile_rows - first_block
    col_slot = tile_cols // group_len // col_devs * group_len + tile_cols % group_len
    row_pick = jnp.where(live, row_slot, 0)
    col_pick = jnp.where(live, col_slot, 0)
    row_put = jnp.where(live, row_slot, slot_count)
    col_put = jnp.where(live, col_slot, set_blocks)
    hub, squares = hub_seeds, None
    for iteration in range(ITERS):
        last = iteration == ITERS - 1
        part = tile_sums(False, set_blocks, row_pick, col_put, hub, tile_blocks, True)
        column_set, squares, own = reduce_set(
            "row", "col", row_devs, col_devs, host_count, iteration, False, part, squares)
        part = tile_sums(True, slot_count, col_pick, row_put, column_set, tile_blocks, True)
        hub, squares, rest = reduce_set(
            "col", "row", col_devs, row_devs, host_count, ITERS + iteration, last, part, squares)
    authority = (own * squares[None]).astype(jnp.bfloat16)
    hub_scores = (hub.astype(jnp.float32) * rest[None]).astype(jnp.bfloat16)
    return (authority, hub_scores)


def solution(mesh):
    return jax.shard_map(
        functools.partial(local, mesh.shape["row"], mesh.shape["col"]),
        mesh=mesh,
        in_specs=(
            P("row", None, None),
            P(("row", "col"), None, None),
            P(("row", "col")),
            P(("row", "col")),
            P(("row", "col")),
            P(),
        ),
        out_specs=(P(("row", "col"), None, None), P("row", None, None)),
        check_vma=False,
    )
```

```python
import functools

import jax
import jax.numpy as jnp
from jax import lax
from jax.experimental import pallas as pl
from jax.experimental.pallas import tpu as pltpu
from jax.sharding import PartitionSpec as P

ITERS = 2
RB_DEV = 16
MESH = pl.DeviceIdType.MESH
MIB = 1 << 20
UNROLL = 128
LIMIT_MIB = 4


def column_of(row):
    k = row.shape[1]
    eye = lax.broadcasted_iota(jnp.int32, (k, k), 0) == lax.broadcasted_iota(jnp.int32, (k, k), 1)
    return jnp.sum(jnp.where(eye, jnp.broadcast_to(row, (k, k)), 0.0), axis=1, keepdims=True)


def row_of(column, lanes):
    k = column.shape[0]
    eye = lax.broadcasted_iota(jnp.int32, (k, lanes), 0) == lax.broadcasted_iota(jnp.int32, (k, lanes), 1)
    return jnp.sum(jnp.where(eye, jnp.broadcast_to(column, (k, lanes)), 0.0), axis=0, keepdims=True)


def tiles_kernel(transposed, pick_ref, put_ref, x_ref, tiles_ref, out_ref, acc):
    step = pl.program_id(0)
    chunk = UNROLL
    blocks = out_ref.shape[0]
    side, k = tiles_ref.shape[1], x_ref.shape[1]
    base = 0 if tiles_ref.shape[0] == chunk else step * chunk

    @pl.when(step == 0)
    def _():
        acc[...] = jnp.zeros_like(acc)

    dims = (((1,), (1,)), ((), ())) if transposed else (((1,), (0,)), ((), ()))

    products = []
    for u in range(0, chunk, 2):
        x = jnp.concatenate([x_ref[pick_ref[step * chunk + u + v]] for v in range(2)], axis=0)
        if transposed:
            both = tiles_ref[pl.ds(base + u, 2)].reshape(2 * side, side)
        else:
            both = jnp.concatenate([tiles_ref[base + u], tiles_ref[base + u + 1]], axis=1)
        product = lax.dot_general(x, both, dims, preferred_element_type=jnp.float32)
        products += [product[:k, :side], product[k:, side:]]
    for u in range(chunk):
        where = put_ref[step * chunk + u]
        acc[where] = acc[where] + products[u]

    @pl.when(step == pl.num_programs(0) - 1)
    def _():
        @pl.loop(0, blocks)
        def _(b):
            out_ref[b] = acc[b].astype(jnp.bfloat16)


def tile_sums(transposed, blocks, pick, put, x, tiles, resident):
    slots, side = tiles.shape[0], tiles.shape[1]
    k = x.shape[1]
    vmem = pl.BlockSpec(memory_space=pltpu.VMEM)
    held = 2 * UNROLL * side * side * 2
    streamed = pl.BlockSpec((UNROLL, side, side), lambda i, *_: (i, 0, 0))
    grid_spec = pltpu.PrefetchScalarGridSpec(
        num_scalar_prefetch=2,
        grid=(slots // UNROLL,),
        in_specs=[vmem, vmem if resident else streamed],
        out_specs=vmem,
        scratch_shapes=[pltpu.VMEM((blocks + 1, k, side), jnp.float32)],
    )
    return pl.pallas_call(
        functools.partial(tiles_kernel, transposed),
        grid_spec=grid_spec,
        out_shape=jax.ShapeDtypeStruct((blocks, k, side), jnp.bfloat16),
        compiler_params=pltpu.CompilerParams(
            vmem_limit_bytes=(0 if resident else held) + (x.size + blocks * k * side * 3) * 2 + LIMIT_MIB * MIB),
        name="hub_tiles" if transposed else "authority_tiles",
    )(pick, put, x, tiles)


def factor_of(squares, hosts, k, side):
    row = 1.0 / jnp.sqrt(squares / hosts + 1.0)
    return jnp.broadcast_to(column_of(row[0:1, :k]), (k, side))


def parts_of(g):
    return 2 if g % 2 == 0 else 1


def reduce_kernel(axis, other, n, m, g, hosts, scaled, final, *refs):
    refs = list(refs)
    part_ref = refs.pop(0)
    sq_ref = refs.pop(0) if scaled else None
    set_ref = refs.pop(0)
    if final:
        before_ref, after_ref = refs.pop(0), refs.pop(0)
    else:
        sq_out_ref, own = refs.pop(0), refs.pop(0)
    pair_in, hop_out, hop_in, sq_before, sq_axis, sq_other = refs[:6]
    refs = refs[6:]
    if final:
        own = refs.pop(0)
    (pair_send, pair_recv, hop_send, hop_recv, near_send, near_recv, far_send, far_recv,
     sqb_send, sqb_recv, sqa_send, sqa_recv, sqo_send, sqo_recv) = refs
    k, side = part_ref.shape[1], part_ref.shape[2]
    me = lax.axis_index(axis)
    mo = lax.axis_index(other)
    lo, hi = me % 2, me // 2
    highs = n // 2
    pair = hi * 2 + (1 - lo)
    waits = []

    def at(index):
        return {axis: index, other: mo}

    def send(src, dst, send_sem, recv_sem, device):
        copy = pltpu.make_async_remote_copy(
            src_ref=src, dst_ref=dst, send_sem=send_sem, recv_sem=recv_sem,
            device_id=device, device_id_type=MESH,
        )
        copy.start()
        waits.append(copy)
        return copy

    barrier = pltpu.get_barrier_semaphore()
    for d in range(1, n):
        pl.semaphore_signal(barrier, inc=1, device_id=at((me + d) % n), device_id_type=MESH)
    if final:
        for d in range(1, m):
            pl.semaphore_signal(barrier, inc=1, device_id={axis: me, other: (mo + d) % m}, device_id_type=MESH)
    pl.semaphore_wait(barrier, n - 1 + (m - 1 if final else 0))

    def group(h, l):
        return pl.ds((h * 2 + l) * g, g)

    parts = parts_of(g)
    width = g // parts

    def part_of(h, l, c):
        return pl.ds((h * 2 + l) * g + c * width, width)

    def piece(c):
        return pl.ds(c * width, width)

    def order(d):
        return (hi + 1 + d) % highs

    pair_copies = [
        send(part_ref.at[part_of(order(d), 1 - lo, c)], pair_in.at[d, piece(c)],
             pair_send.at[d * parts + c], pair_recv.at[d * parts + c], at(pair))
        for d in range(highs) for c in range(parts)
    ]
    sqb_copies = []
    if scaled:
        sq_before[me] = sq_ref[...]
        sqb_copies = [
            send(sq_ref, sq_before.at[me], sqb_send.at[d - 1], sqb_recv.at[d - 1], at((me + d) % n))
            for d in range(1, n)
        ]
    hop_copies = []
    for d in range(highs):
        h = order(d)
        for c in range(parts):
            at_sem = d * parts + c
            pair_copies[at_sem].wait_recv()
            total = part_ref[part_of(h, lo, c)].astype(jnp.float32) + pair_in[d, piece(c)].astype(jnp.float32)
            if d == highs - 1:
                own[piece(c)] = total
            else:
                hop_out[d, piece(c)] = total.astype(jnp.bfloat16)
                hop_copies.append(send(
                    hop_out.at[d, piece(c)], hop_in.at[d, piece(c)],
                    hop_send.at[at_sem], hop_recv.at[at_sem], at(h * 2 + lo)))
    if scaled:
        for copy in sqb_copies:
            copy.wait_recv()
        factor = factor_of(jnp.sum(sq_before[...], axis=0), hosts, k, side)
        if final:
            before_ref[...] = factor
    for copy in hop_copies:
        copy.wait_recv()
    total = own[...]
    for d in range(highs - 1):
        total = total + hop_in[d].astype(jnp.float32)
    if scaled:
        total = total * factor[None]
    own[...] = total
    set_ref[group(hi, lo)] = total.astype(jnp.bfloat16)

    def send_squares():
        squares = jnp.sum(total * total, axis=0)
        sq_axis[me] = jnp.broadcast_to(row_of(jnp.sum(squares, axis=1, keepdims=True), 128), (8, 128))
        return [
            send(sq_axis.at[me], sq_axis.at[me], sqa_send.at[d - 1], sqa_recv.at[d - 1], at((me + d) % n))
            for d in range(1, n)
        ]

    if final:
        sqa_copies = send_squares()
    far_copies = {}

    def to_partner(d, h, c):
        where = part_of(h, lo, c)
        at_sem = d * parts + c
        return send(set_ref.at[where], set_ref.at[where], near_send.at[at_sem], near_recv.at[at_sem], at(pair))

    near_copies = []
    for c in range(parts):
        where = part_of(hi, lo, c)
        for d in range(highs - 1):
            at_sem = d * parts + c
            far_copies[d, c] = send(
                set_ref.at[where], set_ref.at[where], far_send.at[at_sem], far_recv.at[at_sem], at(order(d) * 2 + lo))
        near_copies.append(to_partner(highs - 1, hi, c))
    if not final:
        sqa_copies = send_squares()

    def axis_squares():
        for copy in sqa_copies:
            copy.wait_recv()
        return jnp.sum(sq_axis[...], axis=0)

    sqo_copies = []
    if final:
        sq_other[mo] = axis_squares()
        sqo_copies = [
            send(sq_other.at[mo], sq_other.at[mo], sqo_send.at[d - 1], sqo_recv.at[d - 1], {axis: me, other: (mo + d) % m})
            for d in range(1, m)
        ]
    for c in range(parts):
        for d in range(highs - 1):
            far_copies[d, c].wait_recv()
            near_copies.append(to_partner(d, (hi + highs - 1 - d) % highs, c))
    if final:
        for copy in sqo_copies:
            copy.wait_recv()
        after_ref[...] = factor_of(jnp.sum(sq_other[...], axis=0), hosts, k, side)
    else:
        sq_out_ref[...] = axis_squares()
    for copy in near_copies:
        copy.wait_recv()
    for copy in waits:
        copy.wait_send()


def reduce_set(axis, other, n, m, hosts, collective_id, final, part, squares=None):
    blocks, k, side = part.shape
    g = blocks // n
    highs = n // 2
    vmem = pl.BlockSpec(memory_space=pltpu.VMEM)
    dma = lambda count: pltpu.SemaphoreType.DMA((max(count, 1),))
    scaled = squares is not None
    table = jax.ShapeDtypeStruct((k, side), jnp.float32)
    outs = [jax.ShapeDtypeStruct((blocks, k, side), jnp.bfloat16)]
    scratch = []
    if final:
        outs += [table, table]
        scratch = [pltpu.VMEM((g, k, side), jnp.float32)]
    else:
        outs += [jax.ShapeDtypeStruct((8, 128), jnp.float32), jax.ShapeDtypeStruct((g, k, side), jnp.float32)]
    operands = (part, squares) if scaled else (part,)
    return pl.pallas_call(
        functools.partial(reduce_kernel, axis, other, n, m, g, hosts, scaled, final),
        out_shape=tuple(outs),
        in_specs=[vmem] * len(operands),
        out_specs=(vmem,) * len(outs),
        scratch_shapes=[
            pltpu.VMEM((highs, g, k, side), jnp.bfloat16),
            pltpu.VMEM((max(highs - 1, 1), g, k, side), jnp.bfloat16),
            pltpu.VMEM((max(highs - 1, 1), g, k, side), jnp.bfloat16),
            pltpu.VMEM((n, 8, 128), jnp.float32),
            pltpu.VMEM((n, 8, 128), jnp.float32),
            pltpu.VMEM((m, 8, 128), jnp.float32),
            *scratch,
            *[dma(count * parts_of(g)) for count in (highs, highs, highs - 1, highs - 1) * 2],
            dma(n - 1), dma(n - 1), dma(n - 1), dma(n - 1), dma(m - 1), dma(m - 1),
        ],
        compiler_params=pltpu.CompilerParams(
            collective_id=collective_id, has_side_effects=True, vmem_limit_bytes=6 * part.size * 2 + 4 * MIB),
        name="reduce_" + axis,
    )(*operands)


def local(row_devs, col_devs, hub_seeds, tile_blocks, tile_rows, tile_cols, tile_count, row_blocks):
    own_row = lax.axis_index("row")
    slot_count = hub_seeds.shape[0]
    tile_slots, tile_side = tile_blocks.shape[0], tile_blocks.shape[1]
    group_len = RB_DEV // col_devs
    set_blocks = group_len * row_devs
    host_count = RB_DEV * row_devs * tile_side
    before = jnp.arange(row_devs, dtype=jnp.int32) < own_row
    first_block = jnp.sum(jnp.where(before, row_blocks, 0))
    live = jnp.arange(tile_slots, dtype=jnp.int32) < tile_count[0]
    row_slot = tile_rows - first_block
    col_slot = tile_cols // group_len // col_devs * group_len + tile_cols % group_len
    row_pick = jnp.where(live, row_slot, 0)
    col_pick = jnp.where(live, col_slot, 0)
    row_put = jnp.where(live, row_slot, slot_count)
    col_put = jnp.where(live, col_slot, set_blocks)
    hub, squares = hub_seeds, None
    for iteration in range(ITERS):
        last = iteration == ITERS - 1
        part = tile_sums(False, set_blocks, row_pick, col_put, hub, tile_blocks, True)
        column_set, squares, own = reduce_set(
            "row", "col", row_devs, col_devs, host_count, iteration, False, part, squares)
        part = tile_sums(True, slot_count, col_pick, row_put, column_set, tile_blocks, True)
        hub, squares, rest = reduce_set(
            "col", "row", col_devs, row_devs, host_count, ITERS + iteration, last, part, squares)
    authority = (own * squares[None]).astype(jnp.bfloat16)
    hub_scores = (hub.astype(jnp.float32) * rest[None]).astype(jnp.bfloat16)
    return (authority, hub_scores)


def solution(mesh):
    return jax.shard_map(
        functools.partial(local, mesh.shape["row"], mesh.shape["col"]),
        mesh=mesh,
        in_specs=(
            P("row", None, None),
            P(("row", "col"), None, None),
            P(("row", "col")),
            P(("row", "col")),
            P(("row", "col")),
            P(),
        ),
        out_specs=(P(("row", "col"), None, None), P("row", None, None)),
        check_vma=False,
    )
```

```python
import functools

import jax
import jax.numpy as jnp
from jax import lax
from jax.experimental import pallas as pl
from jax.experimental.pallas import tpu as pltpu
from jax.sharding import PartitionSpec as P

ITERS = 2
RB_DEV = 16
MESH = pl.DeviceIdType.MESH
MIB = 1 << 20
UNROLL = 128
LIMIT_MIB = 4


def column_of(row):
    k = row.shape[1]
    eye = lax.broadcasted_iota(jnp.int32, (k, k), 0) == lax.broadcasted_iota(jnp.int32, (k, k), 1)
    return jnp.sum(jnp.where(eye, jnp.broadcast_to(row, (k, k)), 0.0), axis=1, keepdims=True)


def row_of(column, lanes):
    k = column.shape[0]
    eye = lax.broadcasted_iota(jnp.int32, (k, lanes), 0) == lax.broadcasted_iota(jnp.int32, (k, lanes), 1)
    return jnp.sum(jnp.where(eye, jnp.broadcast_to(column, (k, lanes)), 0.0), axis=0, keepdims=True)


def tiles_kernel(transposed, pick_ref, put_ref, x_ref, tiles_ref, out_ref, acc):
    step = pl.program_id(0)
    chunk = UNROLL
    blocks = out_ref.shape[0]
    side, k = tiles_ref.shape[1], x_ref.shape[1]
    base = 0 if tiles_ref.shape[0] == chunk else step * chunk

    @pl.when(step == 0)
    def _():
        acc[...] = jnp.zeros_like(acc)

    dims = (((1,), (1,)), ((), ())) if transposed else (((1,), (0,)), ((), ()))

    products = []
    for u in range(0, chunk, 2):
        x = jnp.concatenate([x_ref[pick_ref[step * chunk + u + v]] for v in range(2)], axis=0)
        if transposed:
            both = tiles_ref[pl.ds(base + u, 2)].reshape(2 * side, side)
        else:
            both = jnp.concatenate([tiles_ref[base + u], tiles_ref[base + u + 1]], axis=1)
        product = lax.dot_general(x, both, dims, preferred_element_type=jnp.float32)
        products += [product[:k, :side], product[k:, side:]]
    for u in range(chunk):
        where = put_ref[step * chunk + u]
        acc[where] = acc[where] + products[u]

    @pl.when(step == pl.num_programs(0) - 1)
    def _():
        @pl.loop(0, blocks)
        def _(b):
            out_ref[b] = acc[b].astype(jnp.bfloat16)


def tile_sums(transposed, blocks, pick, put, x, tiles, resident):
    slots, side = tiles.shape[0], tiles.shape[1]
    k = x.shape[1]
    vmem = pl.BlockSpec(memory_space=pltpu.VMEM)
    held = 2 * UNROLL * side * side * 2
    streamed = pl.BlockSpec((UNROLL, side, side), lambda i, *_: (i, 0, 0))
    grid_spec = pltpu.PrefetchScalarGridSpec(
        num_scalar_prefetch=2,
        grid=(slots // UNROLL,),
        in_specs=[vmem, vmem if resident else streamed],
        out_specs=vmem,
        scratch_shapes=[pltpu.VMEM((blocks + 1, k, side), jnp.float32)],
    )
    return pl.pallas_call(
        functools.partial(tiles_kernel, transposed),
        grid_spec=grid_spec,
        out_shape=jax.ShapeDtypeStruct((blocks, k, side), jnp.bfloat16),
        compiler_params=pltpu.CompilerParams(
            vmem_limit_bytes=(0 if resident else held) + (x.size + blocks * k * side * 3) * 2 + LIMIT_MIB * MIB),
        name="hub_tiles" if transposed else "authority_tiles",
    )(pick, put, x, tiles)


def factor_of(squares, hosts, k, side):
    row = 1.0 / jnp.sqrt(squares / hosts + 1.0)
    return jnp.broadcast_to(column_of(row[0:1, :k]), (k, side))


def parts_of(g):
    return 4 if g % 4 == 0 else 2 if g % 2 == 0 else 1


def reduce_kernel(axis, other, n, m, g, hosts, scaled, final, *refs):
    refs = list(refs)
    part_ref = refs.pop(0)
    sq_ref = refs.pop(0) if scaled else None
    set_ref = refs.pop(0)
    if final:
        before_ref, after_ref = refs.pop(0), refs.pop(0)
    else:
        sq_out_ref, own = refs.pop(0), refs.pop(0)
    pair_in, hop_out, hop_in, sq_before, sq_axis, sq_other = refs[:6]
    refs = refs[6:]
    if final:
        own = refs.pop(0)
    (pair_send, pair_recv, hop_send, hop_recv, near_send, near_recv, far_send, far_recv,
     sqb_send, sqb_recv, sqa_send, sqa_recv, sqo_send, sqo_recv) = refs
    k, side = part_ref.shape[1], part_ref.shape[2]
    me = lax.axis_index(axis)
    mo = lax.axis_index(other)
    lo, hi = me % 2, me // 2
    highs = n // 2
    pair = hi * 2 + (1 - lo)
    waits = []

    def at(index):
        return {axis: index, other: mo}

    def send(src, dst, send_sem, recv_sem, device):
        copy = pltpu.make_async_remote_copy(
            src_ref=src, dst_ref=dst, send_sem=send_sem, recv_sem=recv_sem,
            device_id=device, device_id_type=MESH,
        )
        copy.start()
        waits.append(copy)
        return copy

    barrier = pltpu.get_barrier_semaphore()
    for d in range(1, n):
        pl.semaphore_signal(barrier, inc=1, device_id=at((me + d) % n), device_id_type=MESH)
    if final:
        for d in range(1, m):
            pl.semaphore_signal(barrier, inc=1, device_id={axis: me, other: (mo + d) % m}, device_id_type=MESH)
    pl.semaphore_wait(barrier, n - 1 + (m - 1 if final else 0))

    def group(h, l):
        return pl.ds((h * 2 + l) * g, g)

    parts = parts_of(g)
    width = g // parts

    def part_of(h, l, c):
        return pl.ds((h * 2 + l) * g + c * width, width)

    def piece(c):
        return pl.ds(c * width, width)

    def order(d):
        return (hi + 1 + d) % highs

    pair_copies = [
        send(part_ref.at[part_of(order(d), 1 - lo, c)], pair_in.at[d, piece(c)],
             pair_send.at[d * parts + c], pair_recv.at[d * parts + c], at(pair))
        for d in range(highs) for c in range(parts)
    ]
    sqb_copies = []
    if scaled:
        sq_before[me] = sq_ref[...]
        sqb_copies = [
            send(sq_ref, sq_before.at[me], sqb_send.at[d - 1], sqb_recv.at[d - 1], at((me + d) % n))
            for d in range(1, n)
        ]
    hop_copies = []
    for d in range(highs):
        h = order(d)
        for c in range(parts):
            at_sem = d * parts + c
            pair_copies[at_sem].wait_recv()
            total = part_ref[part_of(h, lo, c)].astype(jnp.float32) + pair_in[d, piece(c)].astype(jnp.float32)
            if d == highs - 1:
                own[piece(c)] = total
            else:
                hop_out[d, piece(c)] = total.astype(jnp.bfloat16)
                hop_copies.append(send(
                    hop_out.at[d, piece(c)], hop_in.at[d, piece(c)],
                    hop_send.at[at_sem], hop_recv.at[at_sem], at(h * 2 + lo)))
    if scaled:
        for copy in sqb_copies:
            copy.wait_recv()
        factor = factor_of(jnp.sum(sq_before[...], axis=0), hosts, k, side)
        if final:
            before_ref[...] = factor
    for copy in hop_copies:
        copy.wait_recv()
    total = own[...]
    for d in range(highs - 1):
        total = total + hop_in[d].astype(jnp.float32)
    if scaled:
        total = total * factor[None]
    own[...] = total
    set_ref[group(hi, lo)] = total.astype(jnp.bfloat16)

    def send_squares():
        squares = jnp.sum(total * total, axis=0)
        sq_axis[me] = jnp.broadcast_to(row_of(jnp.sum(squares, axis=1, keepdims=True), 128), (8, 128))
        return [
            send(sq_axis.at[me], sq_axis.at[me], sqa_send.at[d - 1], sqa_recv.at[d - 1], at((me + d) % n))
            for d in range(1, n)
        ]

    if final:
        sqa_copies = send_squares()
    far_copies = {}

    def to_partner(d, h, c):
        where = part_of(h, lo, c)
        at_sem = d * parts + c
        return send(set_ref.at[where], set_ref.at[where], near_send.at[at_sem], near_recv.at[at_sem], at(pair))

    near_copies = []
    for c in range(parts):
        where = part_of(hi, lo, c)
        for d in range(highs - 1):
            at_sem = d * parts + c
            far_copies[d, c] = send(
                set_ref.at[where], set_ref.at[where], far_send.at[at_sem], far_recv.at[at_sem], at(order(d) * 2 + lo))
        near_copies.append(to_partner(highs - 1, hi, c))
    if not final:
        sqa_copies = send_squares()

    def axis_squares():
        for copy in sqa_copies:
            copy.wait_recv()
        return jnp.sum(sq_axis[...], axis=0)

    sqo_copies = []
    if final:
        sq_other[mo] = axis_squares()
        sqo_copies = [
            send(sq_other.at[mo], sq_other.at[mo], sqo_send.at[d - 1], sqo_recv.at[d - 1], {axis: me, other: (mo + d) % m})
            for d in range(1, m)
        ]
    for c in range(parts):
        for d in range(highs - 1):
            far_copies[d, c].wait_recv()
            near_copies.append(to_partner(d, (hi + highs - 1 - d) % highs, c))
    if final:
        for copy in sqo_copies:
            copy.wait_recv()
        after_ref[...] = factor_of(jnp.sum(sq_other[...], axis=0), hosts, k, side)
    else:
        sq_out_ref[...] = axis_squares()
    for copy in near_copies:
        copy.wait_recv()
    for copy in waits:
        copy.wait_send()


def reduce_set(axis, other, n, m, hosts, collective_id, final, part, squares=None):
    blocks, k, side = part.shape
    g = blocks // n
    highs = n // 2
    vmem = pl.BlockSpec(memory_space=pltpu.VMEM)
    dma = lambda count: pltpu.SemaphoreType.DMA((max(count, 1),))
    scaled = squares is not None
    table = jax.ShapeDtypeStruct((k, side), jnp.float32)
    outs = [jax.ShapeDtypeStruct((blocks, k, side), jnp.bfloat16)]
    scratch = []
    if final:
        outs += [table, table]
        scratch = [pltpu.VMEM((g, k, side), jnp.float32)]
    else:
        outs += [jax.ShapeDtypeStruct((8, 128), jnp.float32), jax.ShapeDtypeStruct((g, k, side), jnp.float32)]
    operands = (part, squares) if scaled else (part,)
    return pl.pallas_call(
        functools.partial(reduce_kernel, axis, other, n, m, g, hosts, scaled, final),
        out_shape=tuple(outs),
        in_specs=[vmem] * len(operands),
        out_specs=(vmem,) * len(outs),
        scratch_shapes=[
            pltpu.VMEM((highs, g, k, side), jnp.bfloat16),
            pltpu.VMEM((max(highs - 1, 1), g, k, side), jnp.bfloat16),
            pltpu.VMEM((max(highs - 1, 1), g, k, side), jnp.bfloat16),
            pltpu.VMEM((n, 8, 128), jnp.float32),
            pltpu.VMEM((n, 8, 128), jnp.float32),
            pltpu.VMEM((m, 8, 128), jnp.float32),
            *scratch,
            *[dma(count * parts_of(g)) for count in (highs, highs, highs - 1, highs - 1) * 2],
            dma(n - 1), dma(n - 1), dma(n - 1), dma(n - 1), dma(m - 1), dma(m - 1),
        ],
        compiler_params=pltpu.CompilerParams(
            collective_id=collective_id, has_side_effects=True, vmem_limit_bytes=6 * part.size * 2 + 4 * MIB),
        name="reduce_" + axis,
    )(*operands)


def local(row_devs, col_devs, hub_seeds, tile_blocks, tile_rows, tile_cols, tile_count, row_blocks):
    own_row = lax.axis_index("row")
    slot_count = hub_seeds.shape[0]
    tile_slots, tile_side = tile_blocks.shape[0], tile_blocks.shape[1]
    group_len = RB_DEV // col_devs
    set_blocks = group_len * row_devs
    host_count = RB_DEV * row_devs * tile_side
    before = jnp.arange(row_devs, dtype=jnp.int32) < own_row
    first_block = jnp.sum(jnp.where(before, row_blocks, 0))
    live = jnp.arange(tile_slots, dtype=jnp.int32) < tile_count[0]
    row_slot = tile_rows - first_block
    col_slot = tile_cols // group_len // col_devs * group_len + tile_cols % group_len
    row_pick = jnp.where(live, row_slot, 0)
    col_pick = jnp.where(live, col_slot, 0)
    row_put = jnp.where(live, row_slot, slot_count)
    col_put = jnp.where(live, col_slot, set_blocks)
    hub, squares = hub_seeds, None
    for iteration in range(ITERS):
        last = iteration == ITERS - 1
        part = tile_sums(False, set_blocks, row_pick, col_put, hub, tile_blocks, True)
        column_set, squares, own = reduce_set(
            "row", "col", row_devs, col_devs, host_count, iteration, False, part, squares)
        part = tile_sums(True, slot_count, col_pick, row_put, column_set, tile_blocks, True)
        hub, squares, rest = reduce_set(
            "col", "row", col_devs, row_devs, host_count, ITERS + iteration, last, part, squares)
    authority = (own * squares[None]).astype(jnp.bfloat16)
    hub_scores = (hub.astype(jnp.float32) * rest[None]).astype(jnp.bfloat16)
    return (authority, hub_scores)


def solution(mesh):
    return jax.shard_map(
        functools.partial(local, mesh.shape["row"], mesh.shape["col"]),
        mesh=mesh,
        in_specs=(
            P("row", None, None),
            P(("row", "col"), None, None),
            P(("row", "col")),
            P(("row", "col")),
            P(("row", "col")),
            P(),
        ),
        out_specs=(P(("row", "col"), None, None), P("row", None, None)),
        check_vma=False,
    )
```
